512 devices in a mesh: lon: 16 (over z_hi, x, core), lat: 32 (over z_lo, y).
Axes of the slice: x: 4, y: 4, z: 16 (z_hi: 2, z_lo: 8; z = z_hi * 8 + z_lo), core: 2. Of those that a mesh axis runs over, the one named last changes fastest.
Arguments:
- u_vel: float32 [16, 512, 4320], P(None, 'lat', 'lon'), may hold values from -6 to 6
- v_vel: float32 [16, 512, 4320], P(None, 'lat', 'lon'), may hold values from -6 to 6
- u_mask: int32 [16, 512, 4320], P(None, 'lat', 'lon'), may hold values 0 or 1
- v_mask: int32 [16, 512, 4320], P(None, 'lat', 'lon'), may hold values 0 or 1
- t_mask: int32 [16, 512, 4320], P(None, 'lat', 'lon'), may hold values 0 or 1
- bottom: int32 [512, 4320], P('lat', 'lon'), may hold values from 0 to 16
- inv_dx: float32 [512, 4320], P('lat', 'lon'), may hold values from 0.5 to 2
- inv_dy: float32 [512, 4320], P('lat', 'lon'), may hold values from 0.5 to 2
Outputs:
- flux_spectrum: float32 [16, 512, 2160], P(None, ('lat', 'lon'))
The draws below stay inside these ranges and needn't reach their ends.
All inputs are finite; a program needn't handle non-finite values. No bound on the sum of `u_mask` or of `v_mask` or of `t_mask` on one device may be relied on, other than what follows from the above.
Results may differ from the reference program's by a relative error of at most 0.0003.
Values sent between devices are 32-bit elements; how exact they have to be, the bound alone decides.
No kernel may reach another device: no remote copies, remote signals or barrier semaphores. Data moves between devices by JAX's collectives and lax.ppermute only.
A program may use at most 64 MiB of HBM per device.

```python
import math
import jax
import jax.numpy as jnp
from jax import lax

NI = 4320
K = 16
NJ = 512
NM = 2160


def touch_ends(array, rng, low, high):
    index_at = [jax.random.randint(jax.random.fold_in(rng, axis), (), 0, length) for axis, length in enumerate(array.shape)]
    widest = array.shape.index(max(array.shape))
    next_to = index_at[:widest] + [(index_at[widest] + 1) % array.shape[widest]] + index_at[widest + 1:]
    return array.at[tuple(index_at)].set(low).at[tuple(next_to)].set(high)


def level_of(stream_key, shape, split, low, top_value):
    def one(axis_at, blocks):
        steps = jax.random.uniform(jax.random.fold_in(jax.random.fold_in(stream_key, 6), axis_at), (blocks,), jnp.float32, low / len(split), top_value / len(split))
        return jnp.repeat(jnp.exp(steps), shape[axis_at] // blocks).reshape((-1,) + (1,) * (len(shape) - axis_at - 1))

    loudness = one(*split[0])
    for cut in split[1:]:
        loudness = loudness * one(*cut)
    return loudness


def normal_values(stream_key, dims, scale, bound, split=(), kind=jnp.bfloat16):
    values = scale * jax.random.normal(stream_key, dims, jnp.float32)
    if split:
        values = values * level_of(stream_key, dims, split, -0.22, 0.18)
    return jnp.clip(values, -bound, bound).astype(kind)


def setup_inputs(seed: int = 0) -> dict:
    key_of = jax.random.split(jax.random.key(seed), 9)
    u_vel = normal_values(key_of[0], (K, NJ, NI), 1.0, 6.0, ((1, 32), (2, 16)), jnp.float32)
    v_vel = normal_values(key_of[1], (K, NJ, NI), 1.0, 6.0, ((1, 32), (2, 16)), jnp.float32)
    u_mask = touch_ends((jax.random.randint(key_of[2], (K, NJ, NI), 0, 4) < 3).astype(jnp.int32), jax.random.fold_in(key_of[2], 1), 0, 1)
    v_mask = touch_ends((jax.random.randint(key_of[3], (K, NJ, NI), 0, 4) < 3).astype(jnp.int32), jax.random.fold_in(key_of[3], 1), 0, 1)
    t_mask = touch_ends((jax.random.randint(key_of[4], (K, NJ, NI), 0, 4) < 3).astype(jnp.int32), jax.random.fold_in(key_of[4], 1), 0, 1)
    bottom = touch_ends(jax.random.randint(key_of[5], (NJ, NI), 0, K + 1), jax.random.fold_in(key_of[5], 1), 0, K).astype(jnp.int32)
    inv_dx = jnp.clip(jnp.exp(math.log(2.0) - 1.3862944 * jax.random.uniform(key_of[6], (NJ, NI), jnp.float32) ** level_of(key_of[6], (NJ, NI), ((0, 32), (1, 16)), -0.2, 0.2)), 0.5, 2.0)
    inv_dy = jnp.clip(jnp.exp(math.log(2.0) - 1.3862944 * jax.random.uniform(key_of[7], (NJ, NI), jnp.float32) ** level_of(key_of[7], (NJ, NI), ((0, 32), (1, 16)), -0.2, 0.2)), 0.5, 2.0)
    return {"u_vel": u_vel, "v_vel": v_vel, "u_mask": u_mask, "v_mask": v_mask, "t_mask": t_mask, "bottom": bottom, "inv_dx": inv_dx, "inv_dy": inv_dy}


def level_flux(depth_level_fields, bottom, inv_dx, inv_dy):
    zonal_velocity_slice, meridional_velocity_slice, zonal_mask_slice, meridional_mask_slice, tracer_mask_slice, depth_level_index = depth_level_fields
    live_mask = (depth_level_index < bottom).astype(jnp.float32)
    weight = tracer_mask_slice.astype(jnp.float32) * live_mask
    u_masked = zonal_velocity_slice * zonal_mask_slice.astype(jnp.float32)
    meridional_velocity_masked = meridional_velocity_slice * meridional_mask_slice.astype(jnp.float32)

    def extend(field):
        north_row = -field[-1:, ::-1]
        south_row = jnp.zeros_like(field[:1])
        return jnp.concatenate([south_row, field, north_row], axis=0)

    def along_i(field):
        return (jnp.roll(field, -1, axis=1) - jnp.roll(field, 1, axis=1)) * 0.5 * inv_dx

    def along_j(field):
        extended = extend(field)
        return (extended[2:] - extended[:-2]) * 0.5 * inv_dy

    adv_u = weight * (u_masked * along_i(u_masked) + meridional_velocity_masked * along_j(u_masked))
    adv_v = weight * (u_masked * along_i(meridional_velocity_masked) + meridional_velocity_masked * along_j(meridional_velocity_masked))
    spectra = jnp.fft.rfft(jnp.stack([u_masked, meridional_velocity_masked, adv_u, adv_v]), axis=-1)[..., :NM]
    real_part = jnp.real(spectra)
    imag_part = jnp.imag(spectra)
    cross_terms = (real_part[0] * real_part[2] + imag_part[0] * imag_part[2]
                   + real_part[1] * real_part[3] + imag_part[1] * imag_part[3])
    weights_m = jnp.where(jnp.arange(NM) == 0, 1.0, 2.0).astype(jnp.float32)
    return -weights_m[None, :] * cross_terms / NI


def reference(u_vel, v_vel, u_mask, v_mask, t_mask, bottom, inv_dx, inv_dy):
    level_ids = jnp.arange(K, dtype=jnp.int32)

    def one_level(depth_level_fields):
        return level_flux(depth_level_fields, bottom, inv_dx, inv_dy)

    return lax.map(one_level, (u_vel, v_vel, u_mask, v_mask, t_mask, level_ids)).astype(jnp.float32)
```

```python
import math

import jax
import jax.numpy as jnp
import numpy as np
from jax import lax
from jax.experimental import pallas as pl
from jax.experimental.pallas import tpu as pltpu
from jax.sharding import Mesh
from jax.sharding import PartitionSpec as P

LON = ("zh", "x", "c")
LAT = "lat"
LANES = 128
WIDE = 384
NB = 136
NQ = 68
NH = 72
QMAP = (0, 2, 1, 3)


def tables():
    length = 4320
    lanes = np.arange(LANES)
    group = lanes // 32
    wide_q = np.array(QMAP)[group]
    cols = np.arange(NB)
    lane_tw = np.zeros((5, 2, 8, LANES), np.float32)
    point_tw = np.zeros((5, 2, NB, LANES), np.float32)
    for p in range(5):
        a = 2 * math.pi * ((group * p) % 32) / 32
        lane_tw[p, 0] = np.cos(a)
        lane_tw[p, 1] = -np.sin(a)
        b = 2 * math.pi * ((cols[:, None] * (p + 8 * wide_q)[None]) % length) / length
        point_tw[p, 0] = np.cos(b)
        point_tw[p, 1] = -np.sin(b)
    k2 = np.zeros(2 * NH, np.int64)
    k2[:NQ] = np.arange(NQ)
    k2[NH : NH + NQ] = 134 - np.arange(NQ)
    ang = 2 * math.pi * ((k2[:, None] * np.arange(144)[None]) % 135) / 135
    mat = np.concatenate([np.cos(ang), np.sin(ang)])
    mat[:, 135:] = 0.0
    mat = mat.astype(np.float32)
    high = mat.astype(jnp.bfloat16)
    low = (mat - high.astype(np.float32)).astype(jnp.bfloat16)
    scale = np.full((1, 2176), -2.0 / length, np.float32)
    scale[0, 0] = -1.0 / length
    return lane_tw, point_tw, high, low, scale


def lane_ids(rows):
    return lax.broadcasted_iota(jnp.int32, (rows, LANES), 1)


def halves(first, second):
    low = lane_ids(first.shape[0]) < 64
    a = jnp.where(low, first, pltpu.roll(second, 64, 1))
    b = jnp.where(low, pltpu.roll(first, 64, 1), second)
    return a, b


def turned(*sources):
    parts = []
    for t in range(2):
        pieces = [s[f, t, pl.ds(row, 16, stride=16), :] for s, row in sources for f in range(2)]
        parts.append(jnp.concatenate(pieces, axis=0).T)
    return parts[0], parts[1][: NB - LANES]


def mask_kernel(zh_ref, u_ref, v_ref, mu_ref, mv_ref, out_ref, first_ref, last_ref, keep_ref, send_ref, s0, s1):
    low = zh_ref[0] == 0
    zero = jnp.zeros((16, LANES), jnp.float32)
    for f, (val, msk) in enumerate(((u_ref, mu_ref), (v_ref, mv_ref))):
        for level in range(16):
            rows = slice(level * 16, level * 16 + 16)
            out_ref[f, level, :, 256:] = zero
            out_ref[f, level, :, 0:270] = val[level] * msk[level].astype(jnp.float32)
            wide = out_ref[f, level]
            later = pltpu.roll(wide, WIDE - 135, 1)
            for t in range(3):
                s0[f, t, rows, :] = wide[:, t * LANES : (t + 1) * LANES]
            for t in range(2):
                s1[f, t, rows, :] = later[:, t * LANES : (t + 1) * LANES]
        for t in range(3):
            cols = slice(t * LANES, (t + 1) * LANES)
            first_ref[f * 16 : f * 16 + 16, cols] = s0[f, t, pl.ds(0, 16, stride=16), :]
            last_ref[f * 16 : f * 16 + 16, cols] = s0[f, t, pl.ds(15, 16, stride=16), :]
    for x in range(4):
        blocks = []
        for zd in range(2):
            row = zd * 8 + x * 2
            blocks.append(turned((s0, row), (s1, row), (s0, row + 1), (s1, row + 1)))
        for part, rows in enumerate((slice(0, LANES), slice(LANES, NB))):
            keep_ref[x, rows, :] = jnp.where(low, blocks[0][part], blocks[1][part])
            send_ref[x, rows, :] = jnp.where(low, blocks[1][part], blocks[0][part])


def advect_kernel(m_ref, south_ref, north_ref, mirror_ref, t_ref, bottom_ref, dx_ref, dy_ref, out_ref, tmp, s0, s1):
    row = lax.broadcasted_iota(jnp.int32, (16, WIDE), 0)
    lane = lax.broadcasted_iota(jnp.int32, (16, WIDE), 1)
    half_dx = 0.5 * dx_ref[...]
    half_dy = 0.5 * dy_ref[...]
    bottom = bottom_ref[...]
    for level in range(16):
        um = m_ref[0, level]
        vm = m_ref[1, level]
        weight = t_ref[level].astype(jnp.float32) * (level < bottom).astype(jnp.float32)
        coef_x = weight * um[:, :270] * half_dx
        coef_y = weight * vm[:, :270] * half_dy
        tmp[2, :, 0:270] = coef_x
        edge = tmp[2]
        for f, val in enumerate((um, vm)):
            at = f * 16 + level
            south = south_ref[at : at + 1, :]
            north = north_ref[at : at + 1, :] + mirror_ref[at : at + 1, :]
            up = jnp.where(row == 15, north, pltpu.roll(val, 15, 0))
            down = jnp.where(row == 0, south, pltpu.roll(val, 1, 0))
            right = pltpu.roll(val, WIDE - 1, 1)
            left = pltpu.roll(val, 1, 1)
            tmp[f, :, 0:270] = coef_x * (right - left)[:, :270] + coef_y * (up - down)[:, :270]
            adv = tmp[f]
            rows = slice(level * 16, level * 16 + 16)
            low = jnp.where(lane == 135, pltpu.roll(edge, 135, 1), adv)
            high = jnp.where(lane == 135, pltpu.roll(edge, WIDE - 134, 1), pltpu.roll(adv, WIDE - 135, 1))
            for t in range(2):
                s0[f, t, rows, :] = low[:, t * LANES : (t + 1) * LANES]
                s1[f, t, rows, :] = high[:, t * LANES : (t + 1) * LANES]
    for d in range(8):
        out_ref[d, :LANES], out_ref[d, LANES:] = turned((s0, d), (s1, d), (s0, d + 8), (s1, d + 8))


def split_kernel(zh_ref, a_ref, keep_ref, send_ref):
    low = zh_ref[0] == 0
    for x in range(4):
        a, b = halves(a_ref[2 * x], a_ref[2 * x + 1])
        keep_ref[x] = jnp.where(low, a, b)
        send_ref[x] = jnp.where(low, b, a)


def join_kernel(own_ref, other_ref, out_ref):
    for x in range(4):
        out_ref[2 * x], out_ref[2 * x + 1] = halves(own_ref[x], other_ref[x])


def transform(load, lane_tw, point_tw, high, low, work, emit):
    lane = lane_ids(8)
    sign_c = jnp.where(lane < 64, 1.0, -1.0).astype(jnp.float32)
    first_h = (lane % 64) < 32
    sign_h = jnp.where(first_h, 1.0, -1.0).astype(jnp.float32)
    turned = lane >= 96
    r = math.sqrt(0.5)

    def step(i, carry):
        rows = pl.ds(pl.multiple_of(i * 8, 8), 8)
        x = [load(j, rows, i) for j in range(8)]
        s = [x[j] + x[j + 4] for j in range(4)]
        d = [x[j] - x[j + 4] for j in range(4)]
        e0, e1 = s[0] + s[2], s[1] + s[3]
        o = r * (d[1] - d[3])
        q = r * (d[1] + d[3])
        spectrum = (
            (e0 + e1, None),
            (d[0] + o, -(d[2] + q)),
            (s[0] - s[2], s[3] - s[1]),
            (d[0] - o, d[2] - q),
            (e0 - e1, None),
        )
        for p, (re, im) in enumerate(spectrum):
            if im is None:
                if p:
                    re, im = re * lane_tw[p, 0], re * lane_tw[p, 1]
            else:
                c, t = lane_tw[p, 0], lane_tw[p, 1]
                re, im = re * c - im * t, re * t + im * c
            re = re * sign_c + pltpu.roll(re, 64, 1)
            if im is None:
                re, im = jnp.where(turned, 0.0, re), jnp.where(turned, -re, 0.0)
            else:
                im = im * sign_c + pltpu.roll(im, 64, 1)
                re, im = jnp.where(turned, im, re), jnp.where(turned, -re, im)
            re = re * sign_h + jnp.where(first_h, pltpu.roll(re, 96, 1), pltpu.roll(re, 32, 1))
            im = im * sign_h + jnp.where(first_h, pltpu.roll(im, 96, 1), pltpu.roll(im, 32, 1))
            c, t = point_tw[p, 0, rows, :], point_tw[p, 1, rows, :]
            work[p, rows, 0:LANES] = re * c - im * t
            work[p, rows, LANES : 2 * LANES] = re * t + im * c
        return carry

    lax.fori_loop(0, NB // 8, step, 0)
    for p in range(5):
        work[p, NB:144, :] = jnp.zeros((144 - NB, 2 * LANES), jnp.float32)
        full = work[p]
        full_high = full.astype(jnp.bfloat16)
        full_low = (full - full_high.astype(jnp.float32)).astype(jnp.bfloat16)
        dot = lambda a, b: jnp.dot(a, b, preferred_element_type=jnp.float32)
        g = dot(high[...], full_high) + (dot(high[...], full_low) + dot(low[...], full_high))
        cos, sin = g[: 2 * NH], g[2 * NH :]
        emit(p, cos[:, :LANES] + sin[:, LANES:], cos[:, LANES:] - sin[:, :LANES])


def velocity_kernel(a_ref, lane_tw, point_tw, high, low, re_ref, im_ref, edge_ref, blocks, work):
    for x in range(4):
        blocks[x], blocks[x + 4] = halves(a_ref[2 * x], a_ref[2 * x + 1])
    for j in range(8):
        edge_ref[j : j + 1, :] = blocks[j, 0:1, :]
        edge_ref[8 + j : 9 + j, :] = blocks[j, 134:135, :]

    def emit(p, re, im):
        re_ref[p] = re
        im_ref[p] = im

    transform(lambda j, rows, i: blocks[j, rows, :], lane_tw, point_tw, high, low, work, emit)


def flux_kernel(keep_ref, other_ref, edge_ref, fr_ref, fi_ref, lane_tw, point_tw, high, low, scale, out_ref, blocks, work, spread):
    for x in range(4):
        blocks[x] = keep_ref[x]
        blocks[x + 4] = other_ref[x]
    lane = lane_ids(1)
    first_h = (lane % 64) < 32
    for j in range(8):
        coef = blocks[j, 135:136, :]
        before = (j + 7) % 8
        after = (j + 1) % 8
        head = edge_ref[8 + j : 9 + j, :]
        head = jnp.where(lane < 32, pltpu.roll(edge_ref[8 + before : 9 + before, :], 32, 1), pltpu.roll(head, 32, 1))
        tail = edge_ref[j : j + 1, :]
        tail = jnp.where(lane >= 96, pltpu.roll(edge_ref[after : after + 1, :], 96, 1), pltpu.roll(tail, 96, 1))
        blocks[j, 0:1, :] = blocks[j, 0:1, :] - jnp.where(first_h, coef * head, 0.0)
        blocks[j, 134:135, :] = blocks[j, 134:135, :] + jnp.where(first_h, 0.0, coef * tail)

    def emit(p, re, im):
        flux = fr_ref[p] * re + fi_ref[p] * im
        flux = flux + pltpu.roll(flux, LANES - 16, 1)
        for group in range(4):
            k1 = p + 8 * QMAP[group]
            if (p == 0 and k1 == 24) or (p == 4 and k1 > 12):
                continue
            part = pltpu.roll(flux, LANES - 32 * group, 1) if group else flux
            spread[pl.ds(k1, NQ, stride=32), :] = part[:NQ]
            if k1 % 16:
                spread[pl.ds(32 - k1, NQ, stride=32), :] = part[NH : NH + NQ]

    transform(lambda j, rows, i: blocks[j, rows, :], lane_tw, point_tw, high, low, work, emit)
    for t in range(17):
        cols = slice(t * LANES, min((t + 1) * LANES, 2160))
        width = cols.stop - cols.start
        turned = spread[t * LANES : (t + 1) * LANES, :].T[:16] * scale[:, t * LANES : (t + 1) * LANES]
        out_ref[:, 0, cols] = turned[:, :width]


def shape(*dims):
    return jax.ShapeDtypeStruct(dims, jnp.float32)


def vmem(count):
    return [pl.BlockSpec(memory_space=pltpu.VMEM)] * count


SMEM = pl.BlockSpec(memory_space=pltpu.SMEM)


def scratch(*dims):
    return pltpu.VMEM(dims, jnp.float32)


def body(u_vel, v_vel, u_mask, v_mask, t_mask, bottom, inv_dx, inv_dy):
    zh = lax.axis_index("zh").astype(jnp.int32).reshape(1)
    masked, first, last, keep, send = pl.pallas_call(
        mask_kernel,
        out_shape=(shape(2, 16, 16, WIDE), shape(32, WIDE), shape(32, WIDE), shape(4, NB, LANES), shape(4, NB, LANES)),
        in_specs=[SMEM] + vmem(4),
        out_specs=vmem(5),
        scratch_shapes=[scratch(2, 3, 256, LANES), scratch(2, 2, 256, LANES)],
    )(zh, u_vel, v_vel, u_mask, v_mask)
    with jax.named_scope("zuv"):
        other = lax.ppermute(send, "zh", [(0, 1), (1, 0)])
    count = lax.axis_size(LAT)
    ahead = [(i, i + 1) for i in range(count - 1)]
    with jax.named_scope("south"):
        south = lax.ppermute(last, LAT, ahead)
    with jax.named_scope("north"):
        north = lax.ppermute(first, LAT, [(t, s) for s, t in ahead])
    lon = lax.axis_size(LON)
    mirrored = jnp.pad(-jnp.flip(last[:, :270], 1), ((0, 0), (0, WIDE - 270)))
    pairs = [((i + 1) * count - 1, (lon - i) * count - 1) for i in range(lon)]
    with jax.named_scope("mirror"):
        mirror = lax.ppermute(mirrored, (*LON, LAT), pairs)
    adv = pl.pallas_call(
        advect_kernel,
        out_shape=shape(8, NB, LANES),
        in_specs=vmem(8),
        out_specs=vmem(1)[0],
        scratch_shapes=[scratch(3, 16, WIDE), scratch(2, 2, 256, LANES), scratch(2, 2, 256, LANES)],
    )(masked, south, north, mirror, t_mask, bottom, inv_dx, inv_dy)
    adv = lax.all_to_all(adv, ("x", "c"), 0, 0, tiled=True)
    keep_adv, send_adv = pl.pallas_call(
        split_kernel,
        out_shape=(shape(4, NB, LANES), shape(4, NB, LANES)),
        in_specs=[SMEM] + vmem(1),
        out_specs=vmem(2),
    )(zh, adv)
    with jax.named_scope("zadv"):
        other_adv = lax.ppermute(send_adv, "zh", [(0, 1), (1, 0)])
    joined = pl.pallas_call(
        join_kernel,
        out_shape=shape(8, NB, LANES),
        in_specs=vmem(2),
        out_specs=vmem(1)[0],
    )(keep, other)
    joined = lax.all_to_all(joined, ("x", "c"), 0, 0, tiled=True)
    lane_tw, point_tw, high, low, scale = tables()
    re, im, edge = pl.pallas_call(
        velocity_kernel,
        out_shape=(shape(5, 2 * NH, LANES), shape(5, 2 * NH, LANES), shape(16, LANES)),
        in_specs=vmem(5),
        out_specs=vmem(3),
        scratch_shapes=[scratch(8, NB, LANES), scratch(5, 144, 2 * LANES)],
    )(joined, lane_tw, point_tw, high, low)
    return pl.pallas_call(
        flux_kernel,
        out_shape=shape(16, 1, 2160),
        in_specs=vmem(10),
        out_specs=vmem(1)[0],
        scratch_shapes=[scratch(8, NB, LANES), scratch(5, 144, 2 * LANES), scratch(2176, LANES)],
    )(keep_adv, other_adv, edge, re, im, lane_tw, point_tw, high, low, scale)


def solution(mesh):
    torus = Mesh(mesh.devices.reshape(2, 4, 2, mesh.shape["lat"]), ("zh", "x", "c", "lat"))
    level = P(None, "lat", LON)
    plane = P("lat", LON)
    return jax.shard_map(
        body,
        mesh=torus,
        in_specs=(level, level, level, level, level, plane, plane, plane),
        out_specs=P(None, ("lat", *LON), None),
        check_vma=False,
    )
```

```python
import math

import jax
import jax.numpy as jnp
import numpy as np
from jax import lax
from jax.experimental import pallas as pl
from jax.experimental.pallas import tpu as pltpu
from jax.sharding import Mesh
from jax.sharding import PartitionSpec as P

LON = ("zh", "x", "c")
LAT = "lat"
LANES = 128
WIDE = 384
NB = 136
NQ = 68
NH = 72
QMAP = (0, 2, 1, 3)


def tables():
    length = 4320
    lanes = np.arange(LANES)
    group = lanes // 32
    wide_q = np.array(QMAP)[group]
    cols = np.arange(NB)
    lane_tw = np.zeros((5, 2, 8, LANES), np.float32)
    point_tw = np.zeros((5, 2, NB, LANES), np.float32)
    for p in range(5):
        a = 2 * math.pi * ((group * p) % 32) / 32
        lane_tw[p, 0] = np.cos(a)
        lane_tw[p, 1] = -np.sin(a)
        b = 2 * math.pi * ((cols[:, None] * (p + 8 * wide_q)[None]) % length) / length
        point_tw[p, 0] = np.cos(b)
        point_tw[p, 1] = -np.sin(b)
    k2 = np.zeros(2 * NH, np.int64)
    k2[:NQ] = np.arange(NQ)
    k2[NH : NH + NQ] = 134 - np.arange(NQ)
    ang = 2 * math.pi * ((k2[:, None] * np.arange(144)[None]) % 135) / 135
    mat = np.concatenate([np.cos(ang), np.sin(ang)])
    mat[:, 135:] = 0.0
    mat = mat.astype(np.float32)
    high = mat.astype(jnp.bfloat16)
    low = (mat - high.astype(np.float32)).astype(jnp.bfloat16)
    scale = np.full((1, 2176), -2.0 / length, np.float32)
    scale[0, 0] = -1.0 / length
    reverse = np.zeros((WIDE, WIDE), np.float32)
    reverse[np.arange(270), 269 - np.arange(270)] = -1.0
    return lane_tw, point_tw, high, low, scale, reverse.astype(jnp.bfloat16)


def lane_ids(rows):
    return lax.broadcasted_iota(jnp.int32, (rows, LANES), 1)


def halves(first, second):
    low = lane_ids(first.shape[0]) < 64
    a = jnp.where(low, first, pltpu.roll(second, 64, 1))
    b = jnp.where(low, pltpu.roll(first, 64, 1), second)
    return a, b


def turned(*sources):
    parts = []
    for t in range(2):
        pieces = [s[f, t, pl.ds(row, 16, stride=16), :] for s, row in sources for f in range(2)]
        parts.append(jnp.concatenate(pieces, axis=0).T)
    return parts[0], parts[1][: NB - LANES]


def mask_kernel(zh_ref, u_ref, v_ref, mu_ref, mv_ref, out_ref, first_ref, last_ref, keep_ref, send_ref, s0, s1):
    low = zh_ref[0] == 0
    zero = jnp.zeros((16, LANES), jnp.float32)
    for f, (val, msk) in enumerate(((u_ref, mu_ref), (v_ref, mv_ref))):
        for level in range(16):
            rows = slice(level * 16, level * 16 + 16)
            out_ref[f, level, :, 256:] = zero
            out_ref[f, level, :, 0:270] = val[level] * msk[level].astype(jnp.float32)
            wide = out_ref[f, level]
            later = pltpu.roll(wide, WIDE - 135, 1)
            for t in range(3):
                s0[f, t, rows, :] = wide[:, t * LANES : (t + 1) * LANES]
            for t in range(2):
                s1[f, t, rows, :] = later[:, t * LANES : (t + 1) * LANES]
        for t in range(3):
            cols = slice(t * LANES, (t + 1) * LANES)
            first_ref[f * 16 : f * 16 + 16, cols] = s0[f, t, pl.ds(0, 16, stride=16), :]
            last_ref[f * 16 : f * 16 + 16, cols] = s0[f, t, pl.ds(15, 16, stride=16), :]
    for x in range(4):
        blocks = []
        for zd in range(2):
            row = zd * 8 + x * 2
            blocks.append(turned((s0, row), (s1, row), (s0, row + 1), (s1, row + 1)))
        for part, rows in enumerate((slice(0, LANES), slice(LANES, NB))):
            keep_ref[x, rows, :] = jnp.where(low, blocks[0][part], blocks[1][part])
            send_ref[x, rows, :] = jnp.where(low, blocks[1][part], blocks[0][part])


def advect_kernel(m_ref, south_ref, north_ref, mirror_ref, t_ref, bottom_ref, dx_ref, dy_ref, reverse_ref, out_ref, tmp, s0, s1, above):
    row = lax.broadcasted_iota(jnp.int32, (16, WIDE), 0)
    lane = lax.broadcasted_iota(jnp.int32, (16, WIDE), 1)
    half_dx = 0.5 * dx_ref[...]
    half_dy = 0.5 * dy_ref[...]
    bottom = bottom_ref[...]
    rest = mirror_ref[...]
    total = north_ref[...]
    for _ in range(3):
        part = rest.astype(jnp.bfloat16)
        total = total + jnp.dot(part, reverse_ref[...], preferred_element_type=jnp.float32)
        rest = rest - part.astype(jnp.float32)
    above[...] = total
    for level in range(16):
        um = m_ref[0, level]
        vm = m_ref[1, level]
        weight = t_ref[level].astype(jnp.float32) * (level < bottom).astype(jnp.float32)
        coef_x = weight * um[:, :270] * half_dx
        coef_y = weight * vm[:, :270] * half_dy
        tmp[2, :, 0:270] = coef_x
        edge = tmp[2]
        for f, val in enumerate((um, vm)):
            at = f * 16 + level
            south = south_ref[at : at + 1, :]
            north = above[at : at + 1, :]
            up = jnp.where(row == 15, north, pltpu.roll(val, 15, 0))
            down = jnp.where(row == 0, south, pltpu.roll(val, 1, 0))
            right = pltpu.roll(val, WIDE - 1, 1)
            left = pltpu.roll(val, 1, 1)
            tmp[f, :, 0:270] = coef_x * (right - left)[:, :270] + coef_y * (up - down)[:, :270]
            adv = tmp[f]
            rows = slice(level * 16, level * 16 + 16)
            low = jnp.where(lane == 135, pltpu.roll(edge, 135, 1), adv)
            high = jnp.where(lane == 135, pltpu.roll(edge, WIDE - 134, 1), pltpu.roll(adv, WIDE - 135, 1))
            for t in range(2):
                s0[f, t, rows, :] = low[:, t * LANES : (t + 1) * LANES]
                s1[f, t, rows, :] = high[:, t * LANES : (t + 1) * LANES]
    for d in range(8):
        out_ref[d, :LANES], out_ref[d, LANES:] = turned((s0, d), (s1, d), (s0, d + 8), (s1, d + 8))


def split_kernel(zh_ref, a_ref, keep_ref, send_ref):
    low = zh_ref[0] == 0
    for x in range(4):
        a, b = halves(a_ref[2 * x], a_ref[2 * x + 1])
        keep_ref[x] = jnp.where(low, a, b)
        send_ref[x] = jnp.where(low, b, a)


def join_kernel(own_ref, other_ref, out_ref):
    for x in range(4):
        out_ref[2 * x], out_ref[2 * x + 1] = halves(own_ref[x], other_ref[x])


def transform(load, lane_tw, point_tw, high, low, work, emit):
    lane = lane_ids(8)
    sign_c = jnp.where(lane < 64, 1.0, -1.0).astype(jnp.float32)
    first_h = (lane % 64) < 32
    sign_h = jnp.where(first_h, 1.0, -1.0).astype(jnp.float32)
    turned = lane >= 96
    r = math.sqrt(0.5)

    def step(i, carry):
        rows = pl.ds(pl.multiple_of(i * 8, 8), 8)
        x = [load(j, rows, i) for j in range(8)]
        s = [x[j] + x[j + 4] for j in range(4)]
        d = [x[j] - x[j + 4] for j in range(4)]
        e0, e1 = s[0] + s[2], s[1] + s[3]
        o = r * (d[1] - d[3])
        q = r * (d[1] + d[3])
        spectrum = (
            (e0 + e1, None),
            (d[0] + o, -(d[2] + q)),
            (s[0] - s[2], s[3] - s[1]),
            (d[0] - o, d[2] - q),
            (e0 - e1, None),
        )
        for p, (re, im) in enumerate(spectrum):
            if im is None:
                if p:
                    re, im = re * lane_tw[p, 0], re * lane_tw[p, 1]
            else:
                c, t = lane_tw[p, 0], lane_tw[p, 1]
                re, im = re * c - im * t, re * t + im * c
            re = re * sign_c + pltpu.roll(re, 64, 1)
            if im is None:
                re, im = jnp.where(turned, 0.0, re), jnp.where(turned, -re, 0.0)
            else:
                im = im * sign_c + pltpu.roll(im, 64, 1)
                re, im = jnp.where(turned, im, re), jnp.where(turned, -re, im)
            re = re * sign_h + jnp.where(first_h, pltpu.roll(re, 96, 1), pltpu.roll(re, 32, 1))
            im = im * sign_h + jnp.where(first_h, pltpu.roll(im, 96, 1), pltpu.roll(im, 32, 1))
            c, t = point_tw[p, 0, rows, :], point_tw[p, 1, rows, :]
            work[p, rows, 0:LANES] = re * c - im * t
            work[p, rows, LANES : 2 * LANES] = re * t + im * c
        return carry

    lax.fori_loop(0, NB // 8, step, 0)
    for p in range(5):
        work[p, NB:144, :] = jnp.zeros((144 - NB, 2 * LANES), jnp.float32)
        full = work[p]
        full_high = full.astype(jnp.bfloat16)
        full_low = (full - full_high.astype(jnp.float32)).astype(jnp.bfloat16)
        dot = lambda a, b: jnp.dot(a, b, preferred_element_type=jnp.float32)
        g = dot(high[...], full_high) + (dot(high[...], full_low) + dot(low[...], full_high))
        cos, sin = g[: 2 * NH], g[2 * NH :]
        emit(p, cos[:, :LANES] + sin[:, LANES:], cos[:, LANES:] - sin[:, :LANES])


def velocity_kernel(a_ref, lane_tw, point_tw, high, low, re_ref, im_ref, edge_ref, blocks, work):
    for x in range(4):
        blocks[x], blocks[x + 4] = halves(a_ref[2 * x], a_ref[2 * x + 1])
    for j in range(8):
        edge_ref[j : j + 1, :] = blocks[j, 0:1, :]
        edge_ref[8 + j : 9 + j, :] = blocks[j, 134:135, :]

    def emit(p, re, im):
        re_ref[p] = re
        im_ref[p] = im

    transform(lambda j, rows, i: blocks[j, rows, :], lane_tw, point_tw, high, low, work, emit)


def flux_kernel(keep_ref, other_ref, edge_ref, fr_ref, fi_ref, lane_tw, point_tw, high, low, scale, out_ref, blocks, work, spread):
    for x in range(4):
        blocks[x] = keep_ref[x]
        blocks[x + 4] = other_ref[x]
    lane = lane_ids(1)
    first_h = (lane % 64) < 32
    for j in range(8):
        coef = blocks[j, 135:136, :]
        before = (j + 7) % 8
        after = (j + 1) % 8
        head = edge_ref[8 + j : 9 + j, :]
        head = jnp.where(lane < 32, pltpu.roll(edge_ref[8 + before : 9 + before, :], 32, 1), pltpu.roll(head, 32, 1))
        tail = edge_ref[j : j + 1, :]
        tail = jnp.where(lane >= 96, pltpu.roll(edge_ref[after : after + 1, :], 96, 1), pltpu.roll(tail, 96, 1))
        blocks[j, 0:1, :] = blocks[j, 0:1, :] - jnp.where(first_h, coef * head, 0.0)
        blocks[j, 134:135, :] = blocks[j, 134:135, :] + jnp.where(first_h, 0.0, coef * tail)

    def emit(p, re, im):
        flux = fr_ref[p] * re + fi_ref[p] * im
        flux = flux + pltpu.roll(flux, LANES - 16, 1)
        for group in range(4):
            k1 = p + 8 * QMAP[group]
            if (p == 0 and k1 == 24) or (p == 4 and k1 > 12):
                continue
            part = pltpu.roll(flux, LANES - 32 * group, 1) if group else flux
            spread[pl.ds(k1, NQ, stride=32), :] = part[:NQ]
            if k1 % 16:
                spread[pl.ds(32 - k1, NQ, stride=32), :] = part[NH : NH + NQ]

    transform(lambda j, rows, i: blocks[j, rows, :], lane_tw, point_tw, high, low, work, emit)
    for t in range(17):
        cols = slice(t * LANES, min((t + 1) * LANES, 2160))
        width = cols.stop - cols.start
        turned = spread[t * LANES : (t + 1) * LANES, :].T[:16] * scale[:, t * LANES : (t + 1) * LANES]
        out_ref[:, 0, cols] = turned[:, :width]


def result(*dims):
    return pltpu.VMEM(dims, jnp.float32)


def near(*values):
    return [pltpu.with_memory_space_constraint(v, pltpu.VMEM) for v in values]


def vmem(count):
    return [pl.BlockSpec(memory_space=pltpu.VMEM)] * count


SMEM = pl.BlockSpec(memory_space=pltpu.SMEM)


def scratch(*dims):
    return pltpu.VMEM(dims, jnp.float32)


def layer(u_vel, v_vel, u_mask, v_mask, t_mask, bottom, inv_dx, inv_dy):
    zh = lax.axis_index("zh").astype(jnp.int32).reshape(1)
    lane_tw, point_tw, high, low, scale, reverse = tables()
    masked, first, last, keep, send = pl.pallas_call(
        mask_kernel,
        out_shape=(result(2, 16, 16, WIDE), result(32, WIDE), result(32, WIDE), result(4, NB, LANES), result(4, NB, LANES)),
        in_specs=[SMEM] + vmem(4),
        out_specs=vmem(5),
        scratch_shapes=[scratch(2, 3, 256, LANES), scratch(2, 2, 256, LANES)],
    )(zh, u_vel, v_vel, u_mask, v_mask)
    other = lax.ppermute(send, "zh", [(0, 1), (1, 0)])
    count = lax.axis_size(LAT)
    ahead = [(i, i + 1) for i in range(count - 1)]
    south = lax.ppermute(last, LAT, ahead)
    north = lax.ppermute(first, LAT, [(t, s) for s, t in ahead])
    lon = lax.axis_size(LON)
    pairs = [((i + 1) * count - 1, (lon - i) * count - 1) for i in range(lon)]
    mirror = lax.ppermute(last, (*LON, LAT), pairs)
    adv = pl.pallas_call(
        advect_kernel,
        out_shape=result(8, NB, LANES),
        in_specs=vmem(9),
        out_specs=vmem(1)[0],
        scratch_shapes=[scratch(3, 16, WIDE), scratch(2, 2, 256, LANES), scratch(2, 2, 256, LANES), scratch(32, WIDE)],
    )(*near(masked, south, north, mirror), t_mask, bottom, inv_dx, inv_dy, reverse)
    adv = lax.all_to_all(adv, ("x", "c"), 0, 0, tiled=True)
    keep_adv, send_adv = pl.pallas_call(
        split_kernel,
        out_shape=(result(4, NB, LANES), result(4, NB, LANES)),
        in_specs=[SMEM] + vmem(1),
        out_specs=vmem(2),
    )(zh, *near(adv))
    other_adv = lax.ppermute(send_adv, "zh", [(0, 1), (1, 0)])
    joined = pl.pallas_call(
        join_kernel,
        out_shape=result(8, NB, LANES),
        in_specs=vmem(2),
        out_specs=vmem(1)[0],
    )(*near(keep, other))
    joined = lax.all_to_all(joined, ("x", "c"), 0, 0, tiled=True)
    re, im, edge = pl.pallas_call(
        velocity_kernel,
        out_shape=(result(5, 2 * NH, LANES), result(5, 2 * NH, LANES), result(16, LANES)),
        in_specs=vmem(5),
        out_specs=vmem(3),
        scratch_shapes=[scratch(8, NB, LANES), scratch(5, 144, 2 * LANES)],
    )(*near(joined), lane_tw, point_tw, high, low)
    return pl.pallas_call(
        flux_kernel,
        out_shape=jax.ShapeDtypeStruct((16, 1, 2160), jnp.float32),
        in_specs=vmem(10),
        out_specs=vmem(1)[0],
        scratch_shapes=[scratch(8, NB, LANES), scratch(5, 144, 2 * LANES), scratch(2176, LANES)],
    )(*near(keep_adv, other_adv, edge, re, im), lane_tw, point_tw, high, low, scale)


def solution(mesh):
    torus = Mesh(mesh.devices.reshape(2, 4, 2, mesh.shape["lat"]), ("zh", "x", "c", "lat"))
    level = P(None, "lat", LON)
    plane = P("lat", LON)
    return jax.shard_map(
        layer,
        mesh=torus,
        in_specs=(level, level, level, level, level, plane, plane, plane),
        out_specs=P(None, ("lat", *LON), None),
        check_vma=False,
    )
```

```python
import math

import jax
import jax.numpy as jnp
import numpy as np
from jax import lax
from jax.experimental import pallas as pl
from jax.experimental.pallas import tpu as pltpu
from jax.sharding import Mesh
from jax.sharding import PartitionSpec as P

LON = ("zh", "x", "c")
LAT = "lat"
LANES = 128
WIDE = 384
NB = 136
NQ = 68
NH = 72
QMAP = (0, 2, 1, 3)


def tables():
    length = 4320
    lanes = np.arange(LANES)
    group = lanes // 32
    wide_q = np.array(QMAP)[group]
    cols = np.arange(NB)
    lane_tw = np.zeros((5, 2, 8, LANES), np.float32)
    point_tw = np.zeros((5, 2, NB, LANES), np.float32)
    for p in range(5):
        a = 2 * math.pi * ((group * p) % 32) / 32
        lane_tw[p, 0] = np.cos(a)
        lane_tw[p, 1] = -np.sin(a)
        b = 2 * math.pi * ((cols[:, None] * (p + 8 * wide_q)[None]) % length) / length
        point_tw[p, 0] = np.cos(b)
        point_tw[p, 1] = -np.sin(b)
    k2 = np.zeros(2 * NH, np.int64)
    k2[:NQ] = np.arange(NQ)
    k2[NH : NH + NQ] = 134 - np.arange(NQ)
    ang = 2 * math.pi * ((k2[:, None] * np.arange(144)[None]) % 135) / 135
    mat = np.concatenate([np.cos(ang), np.sin(ang)])
    mat[:, 135:] = 0.0
    mat = mat.astype(np.float32)
    high = mat.astype(jnp.bfloat16)
    low = (mat - high.astype(np.float32)).astype(jnp.bfloat16)
    scale = np.full((1, 2176), -2.0 / length, np.float32)
    scale[0, 0] = -1.0 / length
    reverse = np.zeros((WIDE, WIDE), np.float32)
    reverse[np.arange(270), 269 - np.arange(270)] = -1.0
    return lane_tw, point_tw, high, low, scale, reverse.astype(jnp.bfloat16)


def lane_ids(rows):
    return lax.broadcasted_iota(jnp.int32, (rows, LANES), 1)


def halves(first, second):
    low = lane_ids(first.shape[0]) < 64
    a = jnp.where(low, first, pltpu.roll(second, 64, 1))
    b = jnp.where(low, pltpu.roll(first, 64, 1), second)
    return a, b


def turned(*sources):
    parts = []
    for t in range(2):
        pieces = [s[f, t, pl.ds(row, 16, stride=16), :] for s, row in sources for f in range(2)]
        parts.append(jnp.concatenate(pieces, axis=0).T)
    return parts[0], parts[1][: NB - LANES]


def mask_kernel(zh_ref, u_ref, v_ref, mu_ref, mv_ref, out_ref, first_ref, last_ref, keep_ref, send_ref, s0, s1):
    low = zh_ref[0] == 0
    zero = jnp.zeros((16, LANES), jnp.float32)
    for f, (val, msk) in enumerate(((u_ref, mu_ref), (v_ref, mv_ref))):
        for level in range(16):
            rows = slice(level * 16, level * 16 + 16)
            out_ref[f, level, :, 256:] = zero
            out_ref[f, level, :, 0:270] = val[level] * msk[level].astype(jnp.float32)
            wide = out_ref[f, level]
            later = pltpu.roll(wide, WIDE - 135, 1)
            for t in range(3):
                s0[f, t, rows, :] = wide[:, t * LANES : (t + 1) * LANES]
            for t in range(2):
                s1[f, t, rows, :] = later[:, t * LANES : (t + 1) * LANES]
        for t in range(3):
            cols = slice(t * LANES, (t + 1) * LANES)
            first_ref[f * 16 : f * 16 + 16, cols] = s0[f, t, pl.ds(0, 16, stride=16), :]
            last_ref[f * 16 : f * 16 + 16, cols] = s0[f, t, pl.ds(15, 16, stride=16), :]
    for x in range(4):
        blocks = []
        for zd in range(2):
            row = zd * 8 + x * 2
            blocks.append(turned((s0, row), (s1, row), (s0, row + 1), (s1, row + 1)))
        for part, rows in enumerate((slice(0, LANES), slice(LANES, NB))):
            keep_ref[x, rows, :] = jnp.where(low, blocks[0][part], blocks[1][part])
            send_ref[x, rows, :] = jnp.where(low, blocks[1][part], blocks[0][part])


def advect_kernel(m_ref, south_ref, north_ref, mirror_ref, t_ref, bottom_ref, dx_ref, dy_ref, reverse_ref, out_ref, tmp, s0, s1, above):
    row = lax.broadcasted_iota(jnp.int32, (16, WIDE), 0)
    lane = lax.broadcasted_iota(jnp.int32, (16, WIDE), 1)
    half_dx = 0.5 * dx_ref[...]
    half_dy = 0.5 * dy_ref[...]
    bottom = bottom_ref[...]
    rest = mirror_ref[...]
    total = north_ref[...]
    for _ in range(3):
        part = rest.astype(jnp.bfloat16)
        total = total + jnp.dot(part, reverse_ref[...], preferred_element_type=jnp.float32)
        rest = rest - part.astype(jnp.float32)
    above[...] = total
    for level in range(16):
        um = m_ref[0, level]
        vm = m_ref[1, level]
        weight = t_ref[level].astype(jnp.float32) * (level < bottom).astype(jnp.float32)
        coef_x = weight * um[:, :270] * half_dx
        coef_y = weight * vm[:, :270] * half_dy
        tmp[2, :, 0:270] = coef_x
        edge = tmp[2]
        for f, val in enumerate((um, vm)):
            at = f * 16 + level
            south = south_ref[at : at + 1, :]
            north = above[at : at + 1, :]
            up = jnp.where(row == 15, north, pltpu.roll(val, 15, 0))
            down = jnp.where(row == 0, south, pltpu.roll(val, 1, 0))
            right = pltpu.roll(val, WIDE - 1, 1)
            left = pltpu.roll(val, 1, 1)
            tmp[f, :, 0:270] = coef_x * (right - left)[:, :270] + coef_y * (up - down)[:, :270]
            adv = tmp[f]
            rows = slice(level * 16, level * 16 + 16)
            low = jnp.where(lane == 135, pltpu.roll(edge, 135, 1), adv)
            high = jnp.where(lane == 135, pltpu.roll(edge, WIDE - 134, 1), pltpu.roll(adv, WIDE - 135, 1))
            for t in range(2):
                s0[f, t, rows, :] = low[:, t * LANES : (t + 1) * LANES]
                s1[f, t, rows, :] = high[:, t * LANES : (t + 1) * LANES]
    for d in range(8):
        out_ref[d, :LANES], out_ref[d, LANES:] = turned((s0, d), (s1, d), (s0, d + 8), (s1, d + 8))


def split_kernel(zh_ref, a_ref, keep_ref, send_ref):
    low = zh_ref[0] == 0
    for x in range(4):
        a, b = halves(a_ref[2 * x], a_ref[2 * x + 1])
        keep_ref[x] = jnp.where(low, a, b)
        send_ref[x] = jnp.where(low, b, a)


def join_kernel(own_ref, other_ref, out_ref):
    for x in range(4):
        out_ref[2 * x], out_ref[2 * x + 1] = halves(own_ref[x], other_ref[x])


def transform(load, lane_tw, point_tw, high, low, work, emit):
    lane = lane_ids(8)
    sign_c = jnp.where(lane < 64, 1.0, -1.0).astype(jnp.float32)
    first_h = (lane % 64) < 32
    sign_h = jnp.where(first_h, 1.0, -1.0).astype(jnp.float32)
    turned = lane >= 96
    r = math.sqrt(0.5)

    def step(i, carry):
        rows = pl.ds(pl.multiple_of(i * 8, 8), 8)
        x = [load(j, rows, i) for j in range(8)]
        s = [x[j] + x[j + 4] for j in range(4)]
        d = [x[j] - x[j + 4] for j in range(4)]
        e0, e1 = s[0] + s[2], s[1] + s[3]
        o = r * (d[1] - d[3])
        q = r * (d[1] + d[3])
        spectrum = (
            (e0 + e1, None),
            (d[0] + o, -(d[2] + q)),
            (s[0] - s[2], s[3] - s[1]),
            (d[0] - o, d[2] - q),
            (e0 - e1, None),
        )
        for p, (re, im) in enumerate(spectrum):
            if im is None:
                if p:
                    re, im = re * lane_tw[p, 0], re * lane_tw[p, 1]
            else:
                c, t = lane_tw[p, 0], lane_tw[p, 1]
                re, im = re * c - im * t, re * t + im * c
            re = re * sign_c + pltpu.roll(re, 64, 1)
            if im is None:
                re, im = jnp.where(turned, 0.0, re), jnp.where(turned, -re, 0.0)
            else:
                im = im * sign_c + pltpu.roll(im, 64, 1)
                re, im = jnp.where(turned, im, re), jnp.where(turned, -re, im)
            re = re * sign_h + jnp.where(first_h, pltpu.roll(re, 96, 1), pltpu.roll(re, 32, 1))
            im = im * sign_h + jnp.where(first_h, pltpu.roll(im, 96, 1), pltpu.roll(im, 32, 1))
            c, t = point_tw[p, 0, rows, :], point_tw[p, 1, rows, :]
            work[p, rows, 0:LANES] = re * c - im * t
            work[p, rows, LANES : 2 * LANES] = re * t + im * c
        return carry

    lax.fori_loop(0, NB // 8, step, 0)
    for p in range(5):
        work[p, NB:144, :] = jnp.zeros((144 - NB, 2 * LANES), jnp.float32)
        full = work[p]
        full_high = full.astype(jnp.bfloat16)
        full_low = (full - full_high.astype(jnp.float32)).astype(jnp.bfloat16)
        dot = lambda a, b: jnp.dot(a, b, preferred_element_type=jnp.float32)
        g = dot(high[...], full_high) + (dot(high[...], full_low) + dot(low[...], full_high))
        cos, sin = g[: 2 * NH], g[2 * NH :]
        emit(p, cos[:, :LANES] + sin[:, LANES:], cos[:, LANES:] - sin[:, :LANES])


def velocity_kernel(a_ref, lane_tw, point_tw, high, low, re_ref, im_ref, edge_ref, blocks, work):
    for x in range(4):
        blocks[x], blocks[x + 4] = halves(a_ref[2 * x], a_ref[2 * x + 1])
    for j in range(8):
        edge_ref[j : j + 1, :] = blocks[j, 0:1, :]
        edge_ref[8 + j : 9 + j, :] = blocks[j, 134:135, :]

    def emit(p, re, im):
        re_ref[p] = re
        im_ref[p] = im

    transform(lambda j, rows, i: blocks[j, rows, :], lane_tw, point_tw, high, low, work, emit)


def flux_kernel(keep_ref, other_ref, edge_ref, fr_ref, fi_ref, lane_tw, point_tw, high, low, scale, out_ref, blocks, work, spread):
    for x in range(4):
        blocks[x] = keep_ref[x]
        blocks[x + 4] = other_ref[x]
    lane = lane_ids(1)
    first_h = (lane % 64) < 32
    for j in range(8):
        coef = blocks[j, 135:136, :]
        before = (j + 7) % 8
        after = (j + 1) % 8
        head = edge_ref[8 + j : 9 + j, :]
        head = jnp.where(lane < 32, pltpu.roll(edge_ref[8 + before : 9 + before, :], 32, 1), pltpu.roll(head, 32, 1))
        tail = edge_ref[j : j + 1, :]
        tail = jnp.where(lane >= 96, pltpu.roll(edge_ref[after : after + 1, :], 96, 1), pltpu.roll(tail, 96, 1))
        blocks[j, 0:1, :] = blocks[j, 0:1, :] - jnp.where(first_h, coef * head, 0.0)
        blocks[j, 134:135, :] = blocks[j, 134:135, :] + jnp.where(first_h, 0.0, coef * tail)

    def emit(p, re, im):
        flux = fr_ref[p] * re + fi_ref[p] * im
        flux = flux + pltpu.roll(flux, LANES - 16, 1)
        for group in range(4):
            k1 = p + 8 * QMAP[group]
            if (p == 0 and k1 == 24) or (p == 4 and k1 > 12):
                continue
            part = pltpu.roll(flux, LANES - 32 * group, 1) if group else flux
            spread[pl.ds(k1, NQ, stride=32), :] = part[:NQ]
            if k1 % 16:
                spread[pl.ds(32 - k1, NQ, stride=32), :] = part[NH : NH + NQ]

    transform(lambda j, rows, i: blocks[j, rows, :], lane_tw, point_tw, high, low, work, emit)
    for t in range(17):
        cols = slice(t * LANES, min((t + 1) * LANES, 2160))
        width = cols.stop - cols.start
        turned = spread[t * LANES : (t + 1) * LANES, :].T[:16] * scale[:, t * LANES : (t + 1) * LANES]
        out_ref[:, 0, cols] = turned[:, :width]


def result(*dims):
    return pltpu.VMEM(dims, jnp.float32)


def near(*values):
    return [pltpu.with_memory_space_constraint(v, pltpu.VMEM) for v in values]


def far(*values):
    return [pltpu.with_memory_space_constraint(v, pltpu.HBM) for v in values]


def vmem(count):
    return [pl.BlockSpec(memory_space=pltpu.VMEM)] * count


SMEM = pl.BlockSpec(memory_space=pltpu.SMEM)
PARAMS = pltpu.CompilerParams(vmem_limit_bytes=16 * 2**20)


def scratch(*dims):
    return pltpu.VMEM(dims, jnp.float32)


def layer(u_vel, v_vel, u_mask, v_mask, t_mask, bottom, inv_dx, inv_dy):
    zh = lax.axis_index("zh").astype(jnp.int32).reshape(1)
    lane_tw, point_tw, high, low, scale, reverse = (jnp.asarray(t) for t in tables())
    masked, first, last, keep, send = pl.pallas_call(
        mask_kernel,
        compiler_params=PARAMS,
        out_shape=(result(2, 16, 16, WIDE), result(32, WIDE), result(32, WIDE), result(4, NB, LANES), result(4, NB, LANES)),
        in_specs=[SMEM] + vmem(4),
        out_specs=vmem(5),
        scratch_shapes=[scratch(2, 3, 256, LANES), scratch(2, 2, 256, LANES)],
    )(zh, *far(u_vel, v_vel, u_mask, v_mask))
    other = lax.ppermute(send, "zh", [(0, 1), (1, 0)])
    count = lax.axis_size(LAT)
    ahead = [(i, i + 1) for i in range(count - 1)]
    south = lax.ppermute(last, LAT, ahead)
    north = lax.ppermute(first, LAT, [(t, s) for s, t in ahead])
    lon = lax.axis_size(LON)
    pairs = [((i + 1) * count - 1, (lon - i) * count - 1) for i in range(lon)]
    mirror = lax.ppermute(last, (*LON, LAT), pairs)
    adv = pl.pallas_call(
        advect_kernel,
        compiler_params=PARAMS,
        out_shape=result(8, NB, LANES),
        in_specs=vmem(9),
        out_specs=vmem(1)[0],
        scratch_shapes=[scratch(3, 16, WIDE), scratch(2, 2, 256, LANES), scratch(2, 2, 256, LANES), scratch(32, WIDE)],
    )(*near(masked, south, north, mirror, t_mask, bottom, inv_dx, inv_dy, reverse))
    adv = lax.all_to_all(adv, ("x", "c"), 0, 0, tiled=True)
    keep_adv, send_adv = pl.pallas_call(
        split_kernel,
        compiler_params=PARAMS,
        out_shape=(result(4, NB, LANES), result(4, NB, LANES)),
        in_specs=[SMEM] + vmem(1),
        out_specs=vmem(2),
    )(zh, *near(adv))
    other_adv = lax.ppermute(send_adv, "zh", [(0, 1), (1, 0)])
    joined = pl.pallas_call(
        join_kernel,
        compiler_params=PARAMS,
        out_shape=result(8, NB, LANES),
        in_specs=vmem(2),
        out_specs=vmem(1)[0],
    )(*near(keep, other))
    joined = lax.all_to_all(joined, ("x", "c"), 0, 0, tiled=True)
    re, im, edge = pl.pallas_call(
        velocity_kernel,
        compiler_params=PARAMS,
        out_shape=(result(5, 2 * NH, LANES), result(5, 2 * NH, LANES), result(16, LANES)),
        in_specs=vmem(5),
        out_specs=vmem(3),
        scratch_shapes=[scratch(8, NB, LANES), scratch(5, 144, 2 * LANES)],
    )(*near(joined, lane_tw, point_tw, high, low))
    return pl.pallas_call(
        flux_kernel,
        compiler_params=PARAMS,
        out_shape=jax.ShapeDtypeStruct((16, 1, 2160), jnp.float32),
        in_specs=vmem(10),
        out_specs=vmem(1)[0],
        scratch_shapes=[scratch(8, NB, LANES), scratch(5, 144, 2 * LANES), scratch(2176, LANES)],
    )(*near(keep_adv, other_adv, edge, re, im, lane_tw, point_tw, high, low, scale))


def solution(mesh):
    torus = Mesh(mesh.devices.reshape(2, 4, 2, mesh.shape["lat"]), ("zh", "x", "c", "lat"))
    level = P(None, "lat", LON)
    plane = P("lat", LON)
    return jax.shard_map(
        layer,
        mesh=torus,
        in_specs=(level, level, level, level, level, plane, plane, plane),
        out_specs=P(None, ("lat", *LON), None),
        check_vma=False,
    )
```

```python
import math

import jax
import jax.numpy as jnp
import numpy as np
from jax import lax
from jax.experimental import pallas as pl
from jax.experimental.pallas import tpu as pltpu
from jax.sharding import Mesh
from jax.sharding import PartitionSpec as P

LON = ("zh", "x", "c")
LAT = "lat"
LANES = 128
WIDE = 384
NB = 136
NQ = 68
NH = 72
QMAP = (0, 2, 1, 3)
PITCH = 40
UNROLL = 4


def tables():
    length = 4320
    lanes = np.arange(LANES)
    group = lanes // 32
    wide_q = np.array(QMAP)[group]
    cols = np.arange(NB)
    lane_tw = np.zeros((5, 2, 8, LANES), np.float32)
    point_tw = np.zeros((5, 2, NB, LANES), np.float32)
    for p in range(5):
        a = 2 * math.pi * ((group * p) % 32) / 32
        lane_tw[p, 0] = np.cos(a)
        lane_tw[p, 1] = -np.sin(a)
        b = 2 * math.pi * ((cols[:, None] * (p + 8 * wide_q)[None]) % length) / length
        point_tw[p, 0] = np.cos(b)
        point_tw[p, 1] = -np.sin(b)
    k2 = np.zeros(2 * NH, np.int64)
    k2[:NQ] = np.arange(NQ)
    k2[NH : NH + NQ] = 134 - np.arange(NQ)
    ang = 2 * math.pi * ((k2[:, None] * np.arange(144)[None]) % 135) / 135
    mat = np.concatenate([np.cos(ang), np.sin(ang)])
    mat[:, 135:] = 0.0
    mat = mat.astype(np.float32)
    high = mat.astype(jnp.bfloat16)
    low = (mat - high.astype(np.float32)).astype(jnp.bfloat16)
    scale = np.full((1, 2176), -2.0 / length, np.float32)
    scale[0, 0] = -1.0 / length
    reverse = np.zeros((WIDE, WIDE), np.float32)
    reverse[np.arange(270), 269 - np.arange(270)] = -1.0
    return lane_tw, point_tw, high, low, scale, reverse.astype(jnp.bfloat16)


def lane_ids(rows):
    return lax.broadcasted_iota(jnp.int32, (rows, LANES), 1)


def halves(first, second):
    low = lane_ids(first.shape[0]) < 64
    a = jnp.where(low, first, pltpu.roll(second, 64, 1))
    b = jnp.where(low, pltpu.roll(first, 64, 1), second)
    return a, b


def turned(*sources):
    parts = []
    for t in range(2):
        pieces = [s[f, t, pl.ds(row, 16, stride=16), :] for s, row in sources for f in range(2)]
        parts.append(jnp.concatenate(pieces, axis=0).T)
    return parts[0], parts[1][: NB - LANES]


def mask_kernel(zh_ref, u_ref, v_ref, mu_ref, mv_ref, out_ref, first_ref, last_ref, keep_ref, send_ref, s0, s1):
    low = zh_ref[0] == 0
    zero = jnp.zeros((16, LANES), jnp.float32)
    for f, (val, msk) in enumerate(((u_ref, mu_ref), (v_ref, mv_ref))):
        for level in range(16):
            rows = slice(level * 16, level * 16 + 16)
            out_ref[f, level, :, 256:] = zero
            out_ref[f, level, :, 0:270] = val[level] * msk[level].astype(jnp.float32)
            wide = out_ref[f, level]
            later = pltpu.roll(wide, WIDE - 135, 1)
            for t in range(3):
                s0[f, t, rows, :] = wide[:, t * LANES : (t + 1) * LANES]
            for t in range(2):
                s1[f, t, rows, :] = later[:, t * LANES : (t + 1) * LANES]
        for t in range(3):
            cols = slice(t * LANES, (t + 1) * LANES)
            first_ref[f * 16 : f * 16 + 16, cols] = s0[f, t, pl.ds(0, 16, stride=16), :]
            last_ref[f * 16 : f * 16 + 16, cols] = s0[f, t, pl.ds(15, 16, stride=16), :]
    for x in range(4):
        blocks = []
        for zd in range(2):
            row = zd * 8 + x * 2
            blocks.append(turned((s0, row), (s1, row), (s0, row + 1), (s1, row + 1)))
        for part, rows in enumerate((slice(0, LANES), slice(LANES, NB))):
            keep_ref[x, rows, :] = jnp.where(low, blocks[0][part], blocks[1][part])
            send_ref[x, rows, :] = jnp.where(low, blocks[1][part], blocks[0][part])


def advect_kernel(m_ref, south_ref, north_ref, mirror_ref, t_ref, bottom_ref, dx_ref, dy_ref, reverse_ref, out_ref, tmp, s0, s1, above):
    row = lax.broadcasted_iota(jnp.int32, (16, WIDE), 0)
    lane = lax.broadcasted_iota(jnp.int32, (16, WIDE), 1)
    half_dx = 0.5 * dx_ref[...]
    half_dy = 0.5 * dy_ref[...]
    bottom = bottom_ref[...]
    rest = mirror_ref[...]
    total = north_ref[...]
    for _ in range(3):
        part = rest.astype(jnp.bfloat16)
        total = total + jnp.dot(part, reverse_ref[...], preferred_element_type=jnp.float32)
        rest = rest - part.astype(jnp.float32)
    above[...] = total
    for level in range(16):
        um = m_ref[0, level]
        vm = m_ref[1, level]
        weight = t_ref[level].astype(jnp.float32) * (level < bottom).astype(jnp.float32)
        coef_x = weight * um[:, :270] * half_dx
        coef_y = weight * vm[:, :270] * half_dy
        tmp[2, :, 0:270] = coef_x
        edge = tmp[2]
        for f, val in enumerate((um, vm)):
            at = f * 16 + level
            south = south_ref[at : at + 1, :]
            north = above[at : at + 1, :]
            up = jnp.where(row == 15, north, pltpu.roll(val, 15, 0))
            down = jnp.where(row == 0, south, pltpu.roll(val, 1, 0))
            right = pltpu.roll(val, WIDE - 1, 1)
            left = pltpu.roll(val, 1, 1)
            tmp[f, :, 0:270] = coef_x * (right - left)[:, :270] + coef_y * (up - down)[:, :270]
            adv = tmp[f]
            rows = slice(level * 16, level * 16 + 16)
            low = jnp.where(lane == 135, pltpu.roll(edge, 135, 1), adv)
            high = jnp.where(lane == 135, pltpu.roll(edge, WIDE - 134, 1), pltpu.roll(adv, WIDE - 135, 1))
            for t in range(2):
                s0[f, t, rows, :] = low[:, t * LANES : (t + 1) * LANES]
                s1[f, t, rows, :] = high[:, t * LANES : (t + 1) * LANES]
    for d in range(8):
        out_ref[d, :LANES], out_ref[d, LANES:] = turned((s0, d), (s1, d), (s0, d + 8), (s1, d + 8))


def split_kernel(zh_ref, a_ref, keep_ref, send_ref):
    low = zh_ref[0] == 0
    for x in range(4):
        a, b = halves(a_ref[2 * x], a_ref[2 * x + 1])
        keep_ref[x] = jnp.where(low, a, b)
        send_ref[x] = jnp.where(low, b, a)


def join_kernel(own_ref, other_ref, out_ref):
    for x in range(4):
        out_ref[2 * x], out_ref[2 * x + 1] = halves(own_ref[x], other_ref[x])


def transform(load, lane_tw, point_tw, high, low, work, emit):
    lane = lane_ids(8)
    sign_c = jnp.where(lane < 64, 1.0, -1.0).astype(jnp.float32)
    first_h = (lane % 64) < 32
    sign_h = jnp.where(first_h, 1.0, -1.0).astype(jnp.float32)
    turned = lane >= 96
    r = math.sqrt(0.5)

    def step(i, carry):
        rows = pl.ds(pl.multiple_of(i * 8, 8), 8)
        x = [load(j, rows, i) for j in range(8)]
        s = [x[j] + x[j + 4] for j in range(4)]
        d = [x[j] - x[j + 4] for j in range(4)]
        e0, e1 = s[0] + s[2], s[1] + s[3]
        o = r * (d[1] - d[3])
        q = r * (d[1] + d[3])
        spectrum = (
            (e0 + e1, None),
            (d[0] + o, -(d[2] + q)),
            (s[0] - s[2], s[3] - s[1]),
            (d[0] - o, d[2] - q),
            (e0 - e1, None),
        )
        for p, (re, im) in enumerate(spectrum):
            if im is None:
                if p:
                    re, im = re * lane_tw[p, 0], re * lane_tw[p, 1]
            else:
                c, t = lane_tw[p, 0], lane_tw[p, 1]
                re, im = re * c - im * t, re * t + im * c
            re = re * sign_c + pltpu.roll(re, 64, 1)
            if im is None:
                re, im = jnp.where(turned, 0.0, re), jnp.where(turned, -re, 0.0)
            else:
                im = im * sign_c + pltpu.roll(im, 64, 1)
                re, im = jnp.where(turned, im, re), jnp.where(turned, -re, im)
            re = re * sign_h + jnp.where(first_h, pltpu.roll(re, 96, 1), pltpu.roll(re, 32, 1))
            im = im * sign_h + jnp.where(first_h, pltpu.roll(im, 96, 1), pltpu.roll(im, 32, 1))
            c, t = point_tw[p, 0, rows, :], point_tw[p, 1, rows, :]
            work[p, rows, 0:LANES] = re * c - im * t
            work[p, rows, LANES : 2 * LANES] = re * t + im * c
        return carry

    lax.fori_loop(0, NB // 8, step, 0, unroll=UNROLL)
    for p in range(5):
        work[p, NB:144, :] = jnp.zeros((144 - NB, 2 * LANES), jnp.float32)
        full = work[p]
        full_high = full.astype(jnp.bfloat16)
        full_low = (full - full_high.astype(jnp.float32)).astype(jnp.bfloat16)
        dot = lambda a, b: jnp.dot(a, b, preferred_element_type=jnp.float32)
        g = dot(high[...], full_high) + (dot(high[...], full_low) + dot(low[...], full_high))
        cos, sin = g[: 2 * NH], g[2 * NH :]
        emit(p, cos[:, :LANES] + sin[:, LANES:], cos[:, LANES:] - sin[:, :LANES])


def velocity_kernel(a_ref, lane_tw, point_tw, high, low, re_ref, im_ref, edge_ref, blocks, work):
    for x in range(4):
        blocks[x], blocks[x + 4] = halves(a_ref[2 * x], a_ref[2 * x + 1])
    for j in range(8):
        edge_ref[j : j + 1, :] = blocks[j, 0:1, :]
        edge_ref[8 + j : 9 + j, :] = blocks[j, 134:135, :]

    def emit(p, re, im):
        re_ref[p] = re
        im_ref[p] = im

    transform(lambda j, rows, i: blocks[j, rows, :], lane_tw, point_tw, high, low, work, emit)


def flux_kernel(keep_ref, other_ref, edge_ref, fr_ref, fi_ref, lane_tw, point_tw, high, low, scale, out_ref, blocks, work, spread):
    for x in range(4):
        blocks[x] = keep_ref[x]
        blocks[x + 4] = other_ref[x]
    lane = lane_ids(1)
    first_h = (lane % 64) < 32
    for j in range(8):
        coef = blocks[j, 135:136, :]
        before = (j + 7) % 8
        after = (j + 1) % 8
        head = edge_ref[8 + j : 9 + j, :]
        head = jnp.where(lane < 32, pltpu.roll(edge_ref[8 + before : 9 + before, :], 32, 1), pltpu.roll(head, 32, 1))
        tail = edge_ref[j : j + 1, :]
        tail = jnp.where(lane >= 96, pltpu.roll(edge_ref[after : after + 1, :], 96, 1), pltpu.roll(tail, 96, 1))
        blocks[j, 0:1, :] = blocks[j, 0:1, :] - jnp.where(first_h, coef * head, 0.0)
        blocks[j, 134:135, :] = blocks[j, 134:135, :] + jnp.where(first_h, 0.0, coef * tail)

    def emit(p, re, im):
        flux = fr_ref[p] * re + fi_ref[p] * im
        flux = flux + pltpu.roll(flux, LANES - 16, 1)
        for group in range(4):
            k1 = p + 8 * QMAP[group]
            if (p == 0 and k1 == 24) or (p == 4 and k1 > 12):
                continue
            part = pltpu.roll(flux, LANES - 32 * group, 1) if group else flux
            spread[pl.ds(k1, NQ, stride=PITCH), :] = part[:NQ]
            if k1 % 16:
                spread[pl.ds(32 - k1, NQ, stride=PITCH), :] = part[NH : NH + NQ]

    transform(lambda j, rows, i: blocks[j, rows, :], lane_tw, point_tw, high, low, work, emit)
    for t in range(17):
        cols = slice(t * LANES, min((t + 1) * LANES, 2160))
        pieces = [spread[k2 * PITCH : k2 * PITCH + 32, :] for k2 in range(4 * t, 4 * t + 4)]
        piece = jnp.concatenate(pieces, axis=0).T[:16] * scale[:, t * LANES : (t + 1) * LANES]
        out_ref[:, 0, cols] = piece[:, : cols.stop - cols.start]


def result(*dims):
    return pltpu.VMEM(dims, jnp.float32)


def near(*values):
    return [pltpu.with_memory_space_constraint(v, pltpu.VMEM) for v in values]


def far(*values):
    return [pltpu.with_memory_space_constraint(v, pltpu.HBM) for v in values]


def vmem(count):
    return [pl.BlockSpec(memory_space=pltpu.VMEM)] * count


SMEM = pl.BlockSpec(memory_space=pltpu.SMEM)
PARAMS = pltpu.CompilerParams(vmem_limit_bytes=16 * 2**20)


def scratch(*dims):
    return pltpu.VMEM(dims, jnp.float32)


def layer(u_vel, v_vel, u_mask, v_mask, t_mask, bottom, inv_dx, inv_dy):
    zh = lax.axis_index("zh").astype(jnp.int32).reshape(1)
    lane_tw, point_tw, high, low, scale, reverse = (jnp.asarray(t) for t in tables())
    masked, first, last, keep, send = pl.pallas_call(
        mask_kernel,
        compiler_params=PARAMS,
        out_shape=(result(2, 16, 16, WIDE), result(32, WIDE), result(32, WIDE), result(4, NB, LANES), result(4, NB, LANES)),
        in_specs=[SMEM] + vmem(4),
        out_specs=vmem(5),
        scratch_shapes=[scratch(2, 3, 256, LANES), scratch(2, 2, 256, LANES)],
    )(zh, *far(u_vel, v_vel, u_mask, v_mask))
    other = lax.ppermute(send, "zh", [(0, 1), (1, 0)])
    count = lax.axis_size(LAT)
    ahead = [(i, i + 1) for i in range(count - 1)]
    south = lax.ppermute(last, LAT, ahead)
    north = lax.ppermute(first, LAT, [(t, s) for s, t in ahead])
    lon = lax.axis_size(LON)
    pairs = [((i + 1) * count - 1, (lon - i) * count - 1) for i in range(lon)]
    mirror = lax.ppermute(last, (*LON, LAT), pairs)
    adv = pl.pallas_call(
        advect_kernel,
        compiler_params=PARAMS,
        out_shape=result(8, NB, LANES),
        in_specs=vmem(9),
        out_specs=vmem(1)[0],
        scratch_shapes=[scratch(3, 16, WIDE), scratch(2, 2, 256, LANES), scratch(2, 2, 256, LANES), scratch(32, WIDE)],
    )(*near(masked, south, north, mirror, t_mask, bottom, inv_dx, inv_dy, reverse))
    adv = lax.all_to_all(adv, ("x", "c"), 0, 0, tiled=True)
    keep_adv, send_adv = pl.pallas_call(
        split_kernel,
        compiler_params=PARAMS,
        out_shape=(result(4, NB, LANES), result(4, NB, LANES)),
        in_specs=[SMEM] + vmem(1),
        out_specs=vmem(2),
    )(zh, *near(adv))
    other_adv = lax.ppermute(send_adv, "zh", [(0, 1), (1, 0)])
    joined = pl.pallas_call(
        join_kernel,
        compiler_params=PARAMS,
        out_shape=result(8, NB, LANES),
        in_specs=vmem(2),
        out_specs=vmem(1)[0],
    )(*near(keep, other))
    joined = lax.all_to_all(joined, ("x", "c"), 0, 0, tiled=True)
    re, im, edge = pl.pallas_call(
        velocity_kernel,
        compiler_params=PARAMS,
        out_shape=(result(5, 2 * NH, LANES), result(5, 2 * NH, LANES), result(16, LANES)),
        in_specs=vmem(5),
        out_specs=vmem(3),
        scratch_shapes=[scratch(8, NB, LANES), scratch(5, 144, 2 * LANES)],
    )(*near(joined, lane_tw, point_tw, high, low))
    return pl.pallas_call(
        flux_kernel,
        compiler_params=PARAMS,
        out_shape=jax.ShapeDtypeStruct((16, 1, 2160), jnp.float32),
        in_specs=vmem(10),
        out_specs=vmem(1)[0],
        scratch_shapes=[scratch(8, NB, LANES), scratch(5, 144, 2 * LANES), scratch(NQ * PITCH, LANES)],
    )(*near(keep_adv, other_adv, edge, re, im, lane_tw, point_tw, high, low, scale))


def solution(mesh):
    torus = Mesh(mesh.devices.reshape(2, 4, 2, mesh.shape["lat"]), ("zh", "x", "c", "lat"))
    level = P(None, "lat", LON)
    plane = P("lat", LON)
    return jax.shard_map(
        layer,
        mesh=torus,
        in_specs=(level, level, level, level, level, plane, plane, plane),
        out_specs=P(None, ("lat", *LON), None),
        check_vma=False,
    )
```
